32 devices in a mesh: node: 8 (over z, x), rep: 4 (over y, core).
Axes of the slice: x: 2, y: 2, z: 4, core: 2. Of those that a mesh axis runs over, the one named last changes fastest.
Arguments:
- features: bfloat16 [163840, 256], P('node'), may hold values from -6 to 6
- w_in: bfloat16 [256, 256], replicated, may hold values from -0.375 to 0.375
- w_out: bfloat16 [256, 256], replicated, may hold values from -0.375 to 0.375
- pos_src: int32 [8, 4, 8, 2], P('node', 'rep'), may hold values from 0 to 159
- pos_dst: int32 [8, 4, 8, 2], P('node', 'rep'), may hold values from 0 to 159
- counts: int32 [8, 4, 8], P('node', 'rep'), may hold values from 1 to 2, as said below
- neg_blocks: int32 [8, 2], P('node'), may hold values from 0 to 159
- neg_pick: int32 [8, 4, 8, 2], P('node', 'rep'), may hold values from 0 to 15
Outputs:
- pos_scores: float32 [8, 4, 8, 2, 128], P('node', 'rep')
- neg_term: float32 [8, 4, 8, 2, 128], P('node', 'rep')
- loss: float32 [], replicated
The draws below stay inside these ranges and needn't reach their ends.
Inputs may be any that keep to these rules, and one draw needn't show every extreme that they name: `counts`: each entry is at most 2; in every draw one owner receives 2 live slots from every device.
All inputs are finite; a program needn't handle non-finite values.
Results may differ from the reference program's by a relative error of at most 0.0027.
Values may be sent and summed in bfloat16 or wider, within the bound.
A program may use at most 192 MiB of HBM per device.

```python
import jax
import jax.numpy as jnp
from jax import lax

D = 256
HID = 256
BLK = 128
BLOCKS_DEV = 160
CAP = 2
NEG = 2
NODES = 163840
POOL = 16
N_NODE = 8
N_REP = 4


def draw_counts(key, part):
    first = jax.random.fold_in(key, 11)
    second = jax.random.fold_in(key, 12)
    third = jax.random.fold_in(key, 13)
    heat = jax.random.randint(first, (N_NODE,), 0, 3)
    uneven = jax.random.randint(second, (N_NODE, N_REP, N_NODE), 0, 4)
    level = jnp.minimum(CAP, (uneven + heat[None, None, :] + 2) // 2)
    hottest = jax.random.randint(third, (), 0, N_NODE)
    owners = jnp.arange(N_NODE)[None, None, :]
    return jnp.where(owners == hottest, CAP, level).astype(jnp.int32)


def place_ends(entries, own_key, least, largest):
    shape = entries.shape
    place = [jax.random.randint(jax.random.fold_in(own_key, axis), (), 0, shape[axis]) for axis in range(len(shape))]
    entries = entries.at[tuple(place)].set(least)
    longest = shape.index(max(shape))
    place[longest] = (place[longest] + 1) % shape[longest]
    return entries.at[tuple(place)].set(largest)


def shard_levels(stream_key, dims, cuts, low, largest):
    level, own = 1.0, jax.random.fold_in(stream_key, 6)
    for dim, shards_of in cuts:
        heights = jnp.exp(jax.random.uniform(jax.random.fold_in(own, dim), (shards_of,), jnp.float32, low / len(cuts), largest / len(cuts)))
        level = level * jnp.repeat(heights, dims[dim] // shards_of).reshape([-1 if axis == dim else 1 for axis in range(len(dims))])
    return level


def centred(stream_key, shape, spread, limit, split=(), held_as=jnp.bfloat16):
    result = jax.random.normal(stream_key, shape, jnp.float32) * spread
    if len(split) > 0:
        result = shard_levels(stream_key, shape, split, -0.22, 0.18) * result
    return jnp.clip(result, min=-limit, max=limit).astype(held_as)


def setup_inputs(seed: int = 0) -> dict:
    streams_of = jax.random.split(jax.random.key(seed), 9)
    features = centred(streams_of[0], (NODES, D), 1.0, 6.0, ((0, 8),))
    w_in = centred(streams_of[1], (D, HID), D ** -0.5, 0.375)
    w_out = centred(streams_of[2], (HID, D), HID ** -0.5, 0.375)
    pos_src = place_ends(jax.random.randint(streams_of[3], (N_NODE, N_REP, N_NODE, CAP), 0, BLOCKS_DEV), jax.random.fold_in(streams_of[3], 1), 0, BLOCKS_DEV - 1).astype(jnp.int32)
    pos_dst = place_ends(jax.random.randint(streams_of[4], (N_NODE, N_REP, N_NODE, CAP), 0, BLOCKS_DEV), jax.random.fold_in(streams_of[4], 1), 0, BLOCKS_DEV - 1).astype(jnp.int32)
    counts = draw_counts(jax.random.fold_in(streams_of[8], 71), 0)
    neg_blocks = place_ends(jax.random.randint(streams_of[6], (N_NODE, NEG), 0, BLOCKS_DEV), jax.random.fold_in(streams_of[6], 1), 0, BLOCKS_DEV - 1).astype(jnp.int32)
    neg_pick = place_ends(jax.random.randint(streams_of[7], (N_NODE, N_REP, N_NODE, CAP), 0, POOL), jax.random.fold_in(streams_of[7], 1), 0, POOL - 1).astype(jnp.int32)
    return dict(features=features, w_in=w_in, w_out=w_out, pos_src=pos_src, pos_dst=pos_dst, counts=counts, neg_blocks=neg_blocks, neg_pick=neg_pick)


def reference(features, w_in, w_out, pos_src, pos_dst, counts, neg_blocks, neg_pick):
    hidden = jax.nn.silu(jnp.dot(features, w_in, preferred_element_type=jnp.float32)).astype(jnp.bfloat16)
    embed = jnp.dot(hidden, w_out, preferred_element_type=jnp.float32).astype(jnp.bfloat16)
    width = embed.shape[1]
    allblk = embed.reshape(N_NODE, BLOCKS_DEV, BLK, width)
    owner_ids = jnp.arange(N_NODE, dtype=jnp.int32)
    pool = allblk[owner_ids[:, None], neg_blocks].reshape(N_NODE * NEG, BLK, width)
    scale = 1.0 / (width ** 0.5)

    def per_node(index):
        mine = allblk[index]
        source = mine[pos_src[index]].astype(jnp.float32)
        target = allblk[owner_ids[None, :, None], pos_dst[index]].astype(jnp.float32)
        cand = pool[neg_pick[index]].astype(jnp.float32)
        raw_pos = jnp.einsum('rocbd,rocbd->rocb', source, target) * scale
        scores = jnp.einsum('rocbd,rocsd->rocbs', source, cand) * scale
        live = jnp.arange(CAP, dtype=jnp.int32)[None, None, :] < counts[index][:, :, None]
        livex = live[..., None]
        pos_out = jnp.where(livex, raw_pos, 0.0)
        neg_out = jnp.where(livex, jnp.mean(jax.nn.softplus(scores), axis=-1), 0.0)
        pos_loss = jnp.sum(jnp.where(livex, jax.nn.softplus(-raw_pos), 0.0))
        return pos_out, neg_out, pos_loss, jnp.sum(neg_out)

    pos_scores, neg_term, pos_losses, neg_sums = lax.map(per_node, jnp.arange(N_NODE, dtype=jnp.int32))
    total = jnp.sum(counts).astype(jnp.float32)
    loss = (jnp.sum(pos_losses) + jnp.sum(neg_sums)) / (BLK * total)
    return pos_scores, neg_term, loss
```

```python
import jax
import jax.numpy as jnp
from jax import lax
from jax.sharding import PartitionSpec as P

BLK = 128


def encode(rows_in, w_in, w_out):
    hidden = jax.nn.silu(jnp.dot(rows_in, w_in, preferred_element_type=jnp.float32)).astype(
        jnp.bfloat16
    )
    return jnp.dot(hidden, w_out, preferred_element_type=jnp.float32).astype(jnp.bfloat16)


def shards(features, w_in, w_out, pos_src, pos_dst, counts, neg_blocks, neg_pick):
    rows, width = features.shape
    owners = pos_dst.shape[2]
    slots = pos_dst.shape[3]
    blocks = features.reshape(rows // BLK, BLK, width)
    asked_ids = pos_dst.reshape(owners, slots)
    asked = lax.all_to_all(asked_ids, "node", split_axis=0, concat_axis=0, tiled=True)
    offers = neg_blocks.size
    wanted = jnp.concatenate([neg_blocks.reshape(-1), asked.reshape(-1), pos_src.reshape(-1)])
    picked = jnp.take(blocks, wanted, axis=0)
    picked = encode(picked.reshape(-1, width), w_in, w_out).reshape(-1, BLK, width)
    offered = picked[:offers]
    reply = picked[offers:offers + owners * slots].reshape(owners, slots, BLK, width)
    source = picked[offers + owners * slots:].reshape(owners, slots, BLK, width)
    fetched = lax.all_to_all(reply, "node", split_axis=0, concat_axis=0, tiled=True)
    pool = lax.all_gather(offered, "node", axis=0, tiled=True)
    cand = jnp.take(pool, neg_pick.reshape(-1), axis=0).reshape(owners, slots, BLK, width)
    scale = 1.0 / width**0.5
    raw_pos = (
        jnp.einsum("ocbd,ocbd->ocb", source, fetched, preferred_element_type=jnp.float32) * scale
    )
    scores = jnp.einsum("ocbd,ocsd->ocbs", source, cand, preferred_element_type=jnp.float32) * scale
    live = jnp.arange(slots, dtype=jnp.int32)[None, :] < counts.reshape(owners, 1)
    livex = live[..., None]
    pos_out = jnp.where(livex, raw_pos, 0.0)
    neg_out = jnp.where(livex, jnp.mean(jax.nn.softplus(scores), axis=-1), 0.0)
    pos_loss = jnp.sum(jnp.where(livex, jax.nn.softplus(-raw_pos), 0.0))
    totals = lax.psum(
        (pos_loss, jnp.sum(neg_out), jnp.sum(counts).astype(jnp.float32)), ("node", "rep")
    )
    loss = (totals[0] + totals[1]) / (BLK * totals[2])
    return (
        pos_out.reshape(1, 1, owners, slots, BLK),
        neg_out.reshape(1, 1, owners, slots, BLK),
        loss,
    )


def solution(mesh):
    return jax.shard_map(
        shards,
        mesh=mesh,
        in_specs=(
            P("node", None),
            P(),
            P(),
            P("node", "rep", None, None),
            P("node", "rep", None, None),
            P("node", "rep", None),
            P("node", None),
            P("node", "rep", None, None),
        ),
        out_specs=(P("node", "rep", None, None, None), P("node", "rep", None, None, None), P()),
        check_vma=False,
    )
```

```python
import functools

import jax
import jax.numpy as jnp
from jax import lax
from jax.experimental import pallas as pl
from jax.experimental.pallas import tpu as pltpu
from jax.sharding import PartitionSpec as P

BLK = 128
LOADS = 8


def encode(rows_in, w_in, w_out):
    hidden = jax.nn.silu(jnp.dot(rows_in, w_in, preferred_element_type=jnp.float32)).astype(
        jnp.bfloat16
    )
    return jnp.dot(hidden, w_out, preferred_element_type=jnp.float32).astype(jnp.bfloat16)


def softplus(v):
    return jnp.maximum(v, 0.0) + jnp.log1p(jnp.exp(-jnp.abs(v)))


def partner(me, step, n):
    if n & (n - 1):
        return (me + step) % n
    out, bit = 0, 1
    while bit < n:
        out = out + ((me // bit + step // bit) % 2) * bit
        bit *= 2
    return out


def source_of(me, step, n):
    if n & (n - 1):
        return (me + n - step) % n
    return partner(me, step, n)


def mirror(step, n):
    return n - step if n & (n - 1) else step


def kernel(
    n, reps, slots, offers,
    src_ids, dst_ids, counts, neg_ids, picks, asks, features, w_in, w_out,
    pos_out, neg_out, loss_out,
    feat, heard, heard_s, reply, fetched, source, offer_own, pool, mine_sum, node_sums, rep_mine,
    rep_sums,
    load_sem, ask_send, ask_recv, local_sem, rep_send, rep_recv, off_send, off_recv,
    own_sem, fwd_send, fwd_recv, sum_send, sum_recv, all_send, all_recv,
):
    me = lax.axis_index("node")
    rep = lax.axis_index("rep")
    width = feat.shape[2]
    piece = feat.shape[0] // LOADS
    scale = 1.0 / width**0.5
    quarter = pool.shape[2]
    per_block = BLK // quarter

    def to_node(j):
        return {"node": j}

    def to_rep(j):
        return {"rep": j}

    def remote(src, dst, send, recv, where):
        return pltpu.make_async_remote_copy(
            src_ref=src, dst_ref=dst, send_sem=send, recv_sem=recv,
            device_id=where, device_id_type=pl.DeviceIdType.MESH,
        )

    loads = [
        pltpu.make_async_copy(
            features.at[pl.ds(s * piece, piece)], feat.at[pl.ds(s * piece, piece)], load_sem.at[s]
        )
        for s in range(LOADS)
    ]
    for load in loads:
        load.start()

    barrier = pltpu.get_barrier_semaphore()

    @pl.loop(1, n)
    def _(step):
        pl.semaphore_signal(
            barrier, inc=1, device_id=to_node(partner(me, step, n)),
            device_id_type=pl.DeviceIdType.MESH,
        )

    for step in range(1, reps):
        pl.semaphore_signal(
            barrier, inc=1, device_id=to_rep((rep + step) % reps),
            device_id_type=pl.DeviceIdType.MESH,
        )
    pl.semaphore_wait(barrier, n - 1 + reps - 1)

    def ask(step):
        to = partner(me, step, n)
        return remote(asks.at[to], heard.at[step], ask_send.at[step], ask_recv.at[step], to_node(to))

    @pl.loop(1, n)
    def _(i):
        ask(n - i).start()

    for load in loads:
        load.wait()

    wi = w_in[...]
    wo = w_out[...]

    def encoded(ids):
        rows = jnp.concatenate([feat[i] for i in ids], axis=0)
        return encode(rows, wi, wo)

    piece_at = pl.multiple_of((rep % per_block) * quarter, quarter)
    offer_own[...] = encode(feat[neg_ids[rep // per_block], pl.ds(piece_at, quarter)], wi, wo)

    own = encoded([dst_ids[me * slots + c] for c in range(slots)])
    reply[0] = own.reshape(slots, BLK, width)

    def offer(step):
        return remote(
            offer_own, pool.at[rep, me], off_send.at[step], off_recv.at[step],
            to_node(partner(me, step, n)),
        )

    @pl.loop(1, n)
    def _(i):
        offer(n - i).start()

    keep = pltpu.make_async_copy(offer_own, pool.at[rep, me], own_sem)
    keep.start()

    @pl.loop(1, n)
    def _(step):
        ask(step).wait()

    down = pltpu.make_async_copy(heard, heard_s, local_sem)
    down.start()
    down.wait()

    def answer(step):
        return remote(
            reply.at[step], fetched.at[step], rep_send.at[step], rep_recv.at[step],
            to_node(partner(me, step, n)),
        )

    @pl.loop(1, n)
    def _(i):
        step = n - i
        reply[step] = encoded(
            [heard_s[mirror(step, n), 0, c] for c in range(slots)]
        ).reshape(slots, BLK, width)

        @pl.when(i > 1)
        def _():
            answer(step + 1).start()

    @pl.loop(0, n)
    def _(o):
        source[o] = encoded([src_ids[o * slots + c] for c in range(slots)]).reshape(
            slots, BLK, width
        )

        @pl.when(o == 0)
        def _():
            answer(1).start()

    @pl.loop(1, n)
    def _(step):
        offer(step).wait()

    keep.wait()
    forwards = []
    for step in range(1, reps):
        to = (rep + step) % reps
        spot = pool.at[rep]
        forwards.append(remote(spot, spot, fwd_send.at[step - 1], fwd_recv.at[step - 1], to_rep(to)))
    for copy in forwards:
        copy.start()
    for copy in forwards:
        copy.wait()

    contract = (((1,), (1,)), ((), ()))

    def one_negative(o, c):
        pick = picks[o * slots + c]
        home = pick // offers
        first = (pick % offers) * per_block
        cand = jnp.concatenate([pool[first + h, home] for h in range(per_block)], axis=0)
        scores = scale * lax.dot_general(
            cand, source[o, c], contract, preferred_element_type=jnp.float32
        )
        term = jnp.sum(softplus(scores), axis=0, keepdims=True) * (1.0 / BLK)
        return jnp.where(c < counts[o], term, 0.0)

    def negatives(o, total):
        rows = [one_negative(o, c) for c in range(slots)]
        neg_out[o] = jnp.concatenate(rows, axis=0)
        return total + functools.reduce(jnp.add, rows)

    total = lax.fori_loop(0, n, negatives, jnp.zeros((1, BLK), jnp.float32))

    diagonal = lax.broadcasted_iota(jnp.int32, (BLK, BLK), 0) == lax.broadcasted_iota(
        jnp.int32, (BLK, BLK), 1
    )

    def positives(held, step, o, total):
        rows = []
        for c in range(slots):
            every = lax.dot_general(
                held[step, c], source[o, c], contract, preferred_element_type=jnp.float32
            )
            raw = scale * jnp.sum(jnp.where(diagonal, every, 0.0), axis=0, keepdims=True)
            live = c < counts[o]
            rows.append(jnp.where(live, raw, 0.0))
            total = total + jnp.where(live, softplus(-raw), 0.0)
        pos_out[o] = jnp.concatenate(rows, axis=0)
        return total

    total = positives(reply, 0, me, total)

    def arrived(i, total):
        step = n - i
        answer(step).wait()
        return positives(fetched, step, source_of(me, step, n), total)

    total = lax.fori_loop(1, n, arrived, total)

    asked = lax.fori_loop(0, n, lambda o, s: s + counts[o], jnp.int32(0))
    mine_sum[0:1] = total
    mine_sum[1:2] = jnp.full((1, BLK), asked.astype(jnp.float32))

    def tell(step):
        return remote(
            mine_sum, node_sums.at[step], sum_send.at[step], sum_recv.at[step],
            to_node(partner(me, step, n)),
        )

    @pl.loop(1, n)
    def _(i):
        tell(n - i).start()

    @pl.loop(1, n)
    def _(step):
        tell(step).wait()

    rep_mine[...] = lax.fori_loop(
        1, n, lambda step, sums: sums + node_sums[step], mine_sum[...]
    )
    tells = [
        remote(
            rep_mine, rep_sums.at[step], all_send.at[step], all_recv.at[step],
            to_rep((rep + step) % reps),
        )
        for step in range(1, reps)
    ]
    for copy in tells:
        copy.start()
    for copy in tells:
        copy.wait()
    sums = rep_mine[...]
    for step in range(1, reps):
        sums = sums + rep_sums[step]
    loss = jnp.sum(sums[0:1], axis=1, keepdims=True) / (BLK * sums[1:2, 0:1])
    loss_out[...] = loss


def shards(n, reps, features, w_in, w_out, pos_src, pos_dst, counts, neg_blocks, neg_pick):
    rows, width = features.shape
    owners = pos_dst.shape[2]
    slots = pos_dst.shape[3]
    offers = neg_blocks.shape[1]
    blocks = rows // BLK
    smem = pl.BlockSpec(memory_space=pltpu.SMEM)
    vmem = pl.BlockSpec(memory_space=pltpu.VMEM)
    dma = pltpu.SemaphoreType.DMA
    group = pltpu.VMEM((owners, slots, BLK, width), jnp.bfloat16)
    call = pl.pallas_call(
        functools.partial(kernel, n, reps, slots, offers),
        out_shape=(
            jax.ShapeDtypeStruct((owners, slots, BLK), jnp.float32),
            jax.ShapeDtypeStruct((owners, slots, BLK), jnp.float32),
            jax.ShapeDtypeStruct((1, 1), jnp.float32),
        ),
        in_specs=[smem] * 5 + [vmem, pl.BlockSpec(memory_space=pl.ANY), vmem, vmem],
        out_specs=(vmem, vmem, vmem),
        scratch_shapes=[
            pltpu.VMEM((blocks, BLK, width), jnp.bfloat16),
            pltpu.VMEM((n, 1, slots), jnp.int32),
            pltpu.SMEM((n, 1, slots), jnp.int32),
            group,
            group,
            group,
            pltpu.VMEM((offers * BLK // reps, width), jnp.bfloat16),
            pltpu.VMEM((reps, n, offers * BLK // reps, width), jnp.bfloat16),
            pltpu.VMEM((2, BLK), jnp.float32),
            pltpu.VMEM((n, 2, BLK), jnp.float32),
            pltpu.VMEM((2, BLK), jnp.float32),
            pltpu.VMEM((reps, 2, BLK), jnp.float32),
            dma((LOADS,)),
            dma((n,)),
            dma((n,)),
            dma,
            dma((n,)),
            dma((n,)),
            dma((n,)),
            dma((n,)),
            dma,
            dma((reps,)),
            dma((reps,)),
            dma((n,)),
            dma((n,)),
            dma((reps,)),
            dma((reps,)),
        ],
        compiler_params=pltpu.CompilerParams(
            collective_id=0, has_side_effects=True, vmem_limit_bytes=67043328
        ),
    )
    pos, neg, loss = call(
        pos_src.reshape(-1),
        pos_dst.reshape(-1),
        counts.reshape(-1),
        neg_blocks.reshape(-1),
        neg_pick.reshape(-1),
        pos_dst.reshape(owners, 1, slots),
        features.reshape(blocks, BLK, width),
        w_in,
        w_out,
    )
    shape = (1, 1, owners, slots, BLK)
    return pos.reshape(shape), neg.reshape(shape), loss.reshape(())


def solution(mesh):
    return jax.shard_map(
        functools.partial(shards, mesh.shape["node"], mesh.shape["rep"]),
        mesh=mesh,
        in_specs=(
            P("node", None),
            P(),
            P(),
            P("node", "rep", None, None),
            P("node", "rep", None, None),
            P("node", "rep", None),
            P("node", None),
            P("node", "rep", None, None),
        ),
        out_specs=(P("node", "rep", None, None, None), P("node", "rep", None, None, None), P()),
        check_vma=False,
    )
```

```python
import functools

import jax
import jax.numpy as jnp
from jax import lax
from jax.experimental import pallas as pl
from jax.experimental.pallas import tpu as pltpu
from jax.sharding import PartitionSpec as P

BLK = 128
LOADS = 8


def encode(rows_in, w_in, w_out):
    hidden = jax.nn.silu(jnp.dot(rows_in, w_in, preferred_element_type=jnp.float32)).astype(
        jnp.bfloat16
    )
    return jnp.dot(hidden, w_out, preferred_element_type=jnp.float32).astype(jnp.bfloat16)


def softplus(v):
    return jnp.maximum(v, 0.0) + jnp.log1p(jnp.exp(-jnp.abs(v)))


def partner(me, step, n):
    if n & (n - 1):
        return (me + step) % n
    out, bit = 0, 1
    while bit < n:
        out = out + ((me // bit + step // bit) % 2) * bit
        bit *= 2
    return out


def source_of(me, step, n):
    if n & (n - 1):
        return (me + n - step) % n
    return partner(me, step, n)


def mirror(step, n):
    return n - step if n & (n - 1) else step


def kernel(
    n, reps, slots, offers,
    src_ids, dst_ids, counts, neg_ids, picks, asks, features, w_in, w_out,
    pos_out, neg_out, loss_out,
    feat, heard, heard_s, reply, fetched, source, offer_own, pool, mine_sum, node_sums, rep_mine,
    rep_sums,
    load_sem, ask_send, ask_recv, local_sem, rep_send, rep_recv, off_send, off_recv,
    own_sem, near_send, near_recv, fwd_send, fwd_recv, sum_send, sum_recv, all_send, all_recv,
):
    me = lax.axis_index("node")
    rep = lax.axis_index("rep")
    width = feat.shape[2]
    piece = feat.shape[0] // LOADS
    scale = 1.0 / width**0.5
    lows, highs, quarter = pool.shape[1:4]
    low, high = me % lows, me // lows
    per_block = BLK // quarter

    def to_node(j):
        return {"node": j}

    def to_rep(j):
        return {"rep": j}

    def remote(src, dst, send, recv, where):
        return pltpu.make_async_remote_copy(
            src_ref=src, dst_ref=dst, send_sem=send, recv_sem=recv,
            device_id=where, device_id_type=pl.DeviceIdType.MESH,
        )

    loads = [
        pltpu.make_async_copy(
            features.at[pl.ds(s * piece, piece)], feat.at[pl.ds(s * piece, piece)], load_sem.at[s]
        )
        for s in range(LOADS)
    ]
    for load in loads:
        load.start()

    barrier = pltpu.get_barrier_semaphore()

    @pl.loop(1, n)
    def _(step):
        pl.semaphore_signal(
            barrier, inc=1, device_id=to_node(partner(me, step, n)),
            device_id_type=pl.DeviceIdType.MESH,
        )

    for step in range(1, reps):
        pl.semaphore_signal(
            barrier, inc=1, device_id=to_rep((rep + step) % reps),
            device_id_type=pl.DeviceIdType.MESH,
        )
    pl.semaphore_wait(barrier, n - 1 + reps - 1)

    def ask(step):
        to = partner(me, step, n)
        return remote(asks, heard.at[step], ask_send.at[step], ask_recv.at[step], to_node(to))

    @pl.loop(1, n)
    def _(i):
        ask(n - i).start()

    for load in loads:
        load.wait()

    wi = w_in[...]
    wo = w_out[...]

    def encoded(ids):
        rows = jnp.concatenate([feat[i] for i in ids], axis=0)
        return encode(rows, wi, wo)

    piece_at = pl.multiple_of((rep % per_block) * quarter, quarter)
    offer_own[...] = encode(feat[neg_ids[rep // per_block], pl.ds(piece_at, quarter)], wi, wo)

    own = encoded([dst_ids[c, me] for c in range(slots)])
    reply[0] = own.reshape(slots, BLK, width)

    def offer(step):
        return remote(
            offer_own, pool.at[rep, low, high], off_send.at[step], off_recv.at[step],
            to_node(partner(high, step, highs) * lows + low),
        )

    @pl.loop(1, highs)
    def _(i):
        offer(highs - i).start()

    keep = pltpu.make_async_copy(offer_own, pool.at[rep, low, high], own_sem)
    keep.start()

    @pl.loop(1, n)
    def _(step):
        ask(step).wait()

    down = pltpu.make_async_copy(heard, heard_s, local_sem)
    down.start()
    down.wait()

    def answer(step):
        return remote(
            reply.at[step], fetched.at[step], rep_send.at[step], rep_recv.at[step],
            to_node(partner(me, step, n)),
        )

    @pl.loop(1, n)
    def _(i):
        step = n - i
        reply[step] = encoded(
            [heard_s[mirror(step, n), c, me] for c in range(slots)]
        ).reshape(slots, BLK, width)

        @pl.when(i > 1)
        def _():
            answer(step + 1).start()

    @pl.loop(0, n)
    def _(o):
        source[o] = encoded([src_ids[c, o] for c in range(slots)]).reshape(
            slots, BLK, width
        )

        @pl.when(o == 0)
        def _():
            answer(1).start()

    @pl.loop(1, highs)
    def _(step):
        offer(step).wait()

    keep.wait()
    for step in range(1, lows):
        spot = pool.at[rep, low]
        across = remote(
            spot, spot, near_send, near_recv, to_node(high * lows + (low + step) % lows)
        )
        across.start()
        across.wait()
    forwards = []
    for step in range(1, reps):
        to = (rep + step) % reps
        spot = pool.at[rep]
        forwards.append(remote(spot, spot, fwd_send.at[step - 1], fwd_recv.at[step - 1], to_rep(to)))
    for copy in forwards:
        copy.start()
    for copy in forwards:
        copy.wait()

    contract = (((1,), (1,)), ((), ()))

    def one_negative(o, c):
        pick = picks[c, o]
        home = pick // offers
        first = (pick % offers) * per_block
        cand = jnp.concatenate([pool[first + h, home % lows, home // lows] for h in range(per_block)], axis=0)
        scores = scale * lax.dot_general(
            cand, source[o, c], contract, preferred_element_type=jnp.float32
        )
        term = jnp.sum(softplus(scores), axis=0, keepdims=True) * (1.0 / BLK)
        return jnp.where(c < counts[o], term, 0.0)

    def negatives(o, total):
        rows = [one_negative(o, c) for c in range(slots)]
        neg_out[o] = jnp.concatenate(rows, axis=0)
        return total + functools.reduce(jnp.add, rows)

    total = lax.fori_loop(0, n, negatives, jnp.zeros((1, BLK), jnp.float32))

    diagonal = lax.broadcasted_iota(jnp.int32, (BLK, BLK), 0) == lax.broadcasted_iota(
        jnp.int32, (BLK, BLK), 1
    )

    def positives(held, step, o, total):
        rows = []
        for c in range(slots):
            every = lax.dot_general(
                held[step, c], source[o, c], contract, preferred_element_type=jnp.float32
            )
            raw = scale * jnp.sum(jnp.where(diagonal, every, 0.0), axis=0, keepdims=True)
            live = c < counts[o]
            rows.append(jnp.where(live, raw, 0.0))
            total = total + jnp.where(live, softplus(-raw), 0.0)
        pos_out[o] = jnp.concatenate(rows, axis=0)
        return total

    total = positives(reply, 0, me, total)

    def arrived(i, total):
        step = n - i
        answer(step).wait()
        return positives(fetched, step, source_of(me, step, n), total)

    total = lax.fori_loop(1, n, arrived, total)

    asked = lax.fori_loop(0, n, lambda o, s: s + counts[o], jnp.int32(0))
    mine_sum[0:1] = total
    mine_sum[1:2] = jnp.full((1, BLK), asked.astype(jnp.float32))

    def tell(step):
        return remote(
            mine_sum, node_sums.at[step], sum_send.at[step], sum_recv.at[step],
            to_node(partner(me, step, n)),
        )

    @pl.loop(1, n)
    def _(i):
        tell(n - i).start()

    @pl.loop(1, n)
    def _(step):
        tell(step).wait()

    rep_mine[...] = lax.fori_loop(
        1, n, lambda step, sums: sums + node_sums[step], mine_sum[...]
    )
    tells = [
        remote(
            rep_mine, rep_sums.at[step], all_send.at[step], all_recv.at[step],
            to_rep((rep + step) % reps),
        )
        for step in range(1, reps)
    ]
    for copy in tells:
        copy.start()
    for copy in tells:
        copy.wait()
    sums = rep_mine[...]
    for step in range(1, reps):
        sums = sums + rep_sums[step]
    loss = jnp.sum(sums[0:1], axis=1, keepdims=True) / (BLK * sums[1:2, 0:1])
    loss_out[...] = loss


def shards(n, reps, features, w_in, w_out, pos_src, pos_dst, counts, neg_blocks, neg_pick):
    rows, width = features.shape
    owners = pos_dst.shape[2]
    slots = pos_dst.shape[3]
    offers = neg_blocks.shape[1]
    blocks = rows // BLK
    lows = 1 if n % 2 else 2
    smem = pl.BlockSpec(memory_space=pltpu.SMEM)
    vmem = pl.BlockSpec(memory_space=pltpu.VMEM)
    dma = pltpu.SemaphoreType.DMA
    group = pltpu.VMEM((owners, slots, BLK, width), jnp.bfloat16)

    def by_slot(ids):
        return jnp.swapaxes(ids, 2, 3).reshape(slots, owners)

    call = pl.pallas_call(
        functools.partial(kernel, n, reps, slots, offers),
        out_shape=(
            jax.ShapeDtypeStruct((owners, slots, BLK), jnp.float32),
            jax.ShapeDtypeStruct((owners, slots, BLK), jnp.float32),
            jax.ShapeDtypeStruct((1, 1), jnp.float32),
        ),
        in_specs=[smem] * 5 + [vmem, pl.BlockSpec(memory_space=pl.ANY), vmem, vmem],
        out_specs=(vmem, vmem, vmem),
        scratch_shapes=[
            pltpu.VMEM((blocks, BLK, width), jnp.bfloat16),
            pltpu.VMEM((n, slots, owners), jnp.int32),
            pltpu.SMEM((n, slots, owners), jnp.int32),
            group,
            group,
            group,
            pltpu.VMEM((offers * BLK // reps, width), jnp.bfloat16),
            pltpu.VMEM((reps, lows, n // lows, offers * BLK // reps, width), jnp.bfloat16),
            pltpu.VMEM((2, BLK), jnp.float32),
            pltpu.VMEM((n, 2, BLK), jnp.float32),
            pltpu.VMEM((2, BLK), jnp.float32),
            pltpu.VMEM((reps, 2, BLK), jnp.float32),
            dma((LOADS,)),
            dma((n,)),
            dma((n,)),
            dma,
            dma((n,)),
            dma((n,)),
            dma((n,)),
            dma((n,)),
            dma,
            dma,
            dma,
            dma((reps,)),
            dma((reps,)),
            dma((n,)),
            dma((n,)),
            dma((reps,)),
            dma((reps,)),
        ],
        compiler_params=pltpu.CompilerParams(
            collective_id=0, has_side_effects=True, vmem_limit_bytes=67043328
        ),
    )
    pos, neg, loss = call(
        by_slot(pos_src),
        by_slot(pos_dst),
        counts.reshape(-1),
        neg_blocks.reshape(-1),
        by_slot(neg_pick),
        by_slot(pos_dst),
        features.reshape(blocks, BLK, width),
        w_in,
        w_out,
    )
    shape = (1, 1, owners, slots, BLK)
    return pos.reshape(shape), neg.reshape(shape), loss.reshape(())


def solution(mesh):
    return jax.shard_map(
        functools.partial(shards, mesh.shape["node"], mesh.shape["rep"]),
        mesh=mesh,
        in_specs=(
            P("node", None),
            P(),
            P(),
            P("node", "rep", None, None),
            P("node", "rep", None, None),
            P("node", "rep", None),
            P("node", None),
            P("node", "rep", None, None),
        ),
        out_specs=(P("node", "rep", None, None, None), P("node", "rep", None, None, None), P()),
        check_vma=False,
    )
```
